16 devices in a mesh: rep: 2 (over y, z), dp: 8 (over x, core).
Axes of the slice: x: 4, y: 2, z: 1, core: 2. Of those that a mesh axis runs over, the one named last changes fastest.
The devices are a block of a 4x4x8 slice.
Arguments:
- x: bfloat16 [16, 1024, 512], P(('rep', 'dp')), parts along dimension 0
- dy: bfloat16 [16, 1024, 512], P(('rep', 'dp')), parts along dimension 0
- w_gate: bfloat16 [2, 512, 8192], replicated
- w_up: bfloat16 [2, 512, 8192], replicated
- w_down: bfloat16 [2, 8192, 512], replicated
- m_w_gate: float32 [2, 512, 8192], P(None, 'dp')
- m_w_up: float32 [2, 512, 8192], P(None, 'dp')
- m_w_down: float32 [2, 8192, 512], P(None, 'dp')
- v_w_gate: float32 [2, 512, 8192], P(None, 'dp')
- v_w_up: float32 [2, 512, 8192], P(None, 'dp')
- v_w_down: float32 [2, 8192, 512], P(None, 'dp')
Outputs:
- output 1: bfloat16 [4, 512, 8192], P('rep'), parts along dimension 0
- output 2: bfloat16 [4, 512, 8192], P('rep'), parts along dimension 0
- output 3: bfloat16 [4, 8192, 512], P('rep'), parts along dimension 0
- output 4: float32 [4, 512, 8192], P('rep', 'dp'), parts along dimension 0
- output 5: float32 [4, 512, 8192], P('rep', 'dp'), parts along dimension 0
- output 6: float32 [4, 8192, 512], P('rep', 'dp'), parts along dimension 0
- output 7: float32 [4, 512, 8192], P('rep', 'dp'), parts along dimension 0
- output 8: float32 [4, 512, 8192], P('rep', 'dp'), parts along dimension 0
- output 9: float32 [4, 8192, 512], P('rep', 'dp'), parts along dimension 0
There are 2 independent parts. The reference program is written for one: setup_inputs(seed, part) draws one part's arguments, and reference() takes and returns one part's arrays. A program takes and returns all parts, laid end to end along the dimension named above; an argument that names none is the same for every part.
All inputs are finite; a program needn't handle non-finite values.
Results may differ from the reference program's by a relative error of at most 0.022.
Values are sent between devices in bfloat16 or wider.
A program may use at most 768 MiB of HBM per device.

```python
import jax
import jax.numpy as jnp
from jax import lax

SEQUENCES = 8
TOKENS = 1024
D = 512
FF = 8192
LAYERS = 2
NAMES = ("w_gate", "w_up", "w_down")
SHAPES = {"w_gate": (LAYERS, D, FF), "w_up": (LAYERS, D, FF), "w_down": (LAYERS, FF, D)}


def bump(key, n, height):
    away = (jnp.arange(n, dtype=jnp.int32) - jax.random.randint(key, (), 0, n, jnp.int32)) % n
    return jnp.where(away < n // 8, height, 1.0)


def together(key, own, strength):
    shared = jax.random.normal(key, own.shape[1:], jnp.float32)
    return (own + strength * shared) * lax.rsqrt(1 + strength * strength)


def setup_inputs(seed: int = 0, part: int = 0) -> dict:
    kx, kdy, ka, kb, kz, kf, kh, kl, *keys = jax.random.split(jax.random.key(seed), 8 + 3 * len(NAMES))
    kx, kdy, ka, kb = (jax.random.fold_in(k, part) for k in (kx, kdy, ka, kb))
    kw, km, kv = (keys[i::3] for i in range(3))
    shape = (SEQUENCES, TOKENS, D)
    much_x, much_dy = jax.random.uniform(kz, (2,), jnp.float32, 0.0, 1.0)
    loud = 2.0 ** jax.random.uniform(jax.random.fold_in(kz, 1), (), jnp.float32, -1.0, 2.0)
    layers = 2.0 ** jax.random.uniform(kl, (LAYERS, 1, 1), jnp.float32, -1.0, 1.0)
    x = together(ka, jax.random.normal(kx, shape, jnp.float32), much_x) * bump(kf, D, 4.0)
    dy = together(kb, jax.random.normal(kdy, shape, jnp.float32), much_dy)
    drawn = {"x": x.astype(jnp.bfloat16), "dy": (loud * dy * (SEQUENCES * TOKENS) ** -0.5).astype(jnp.bfloat16)}
    for key, name in zip(kw, NAMES, strict=True):
        w = jax.random.normal(key, SHAPES[name], jnp.float32) * SHAPES[name][1] ** -0.5
        drawn[name] = (w * {"w_gate": 1.0, "w_up": bump(kh, FF, 4.0), "w_down": layers}[name]).astype(jnp.bfloat16)
    for key, name in zip(km, NAMES, strict=True):
        drawn[f"m_{name}"] = 0.1 * jax.random.normal(key, SHAPES[name], jnp.float32)
    for key, name in zip(kv, NAMES, strict=True):
        drawn[f"v_{name}"] = jax.random.uniform(key, SHAPES[name], jnp.float32, 0.005, 0.015)
    return drawn


def matmul(a, w):
    return jnp.dot(a, w, preferred_element_type=jnp.float32).astype(jnp.bfloat16)


def normed(h):
    wide = h.astype(jnp.float32)
    scale = lax.rsqrt(jnp.mean(wide**2, -1, keepdims=True) + 1e-6)
    return (wide * scale).astype(jnp.bfloat16)


def layer(h, w):
    a = normed(h)
    gate = jnp.dot(a, w["w_gate"], preferred_element_type=jnp.float32)
    up = jnp.dot(a, w["w_up"], preferred_element_type=jnp.float32)
    return h + matmul((jax.nn.silu(gate) * up).astype(jnp.bfloat16), w["w_down"])


def adamw(w, m, v, g):
    m = 0.9 * m + 0.1 * g
    v = 0.95 * v + 0.05 * g * g
    step = m * lax.rsqrt(v + 1e-8) + 0.1 * w
    return (w - 0.02 * step).astype(jnp.bfloat16), m, v


def clipped(gradients, sum_of_squares, count):
    factor = jnp.minimum(1.0, 0.5 * lax.rsqrt(sum_of_squares / count + 1e-30))
    return [g * factor for g in gradients]


def stack(weights, h):
    return lax.scan(lambda h, w: (layer(h, w), None), h, weights)[0]


def reference(x, dy, w_gate, w_up, w_down, m_w_gate, m_w_up, m_w_down, v_w_gate, v_w_up, v_w_down):
    weights = dict(zip(NAMES, (w_gate, w_up, w_down), strict=True))

    def take(so_far, sequence):
        h, by_y = sequence
        _, back = jax.vjp(lambda w: stack(w, h), weights)
        return jax.tree.map(lambda total, term: total + term.astype(jnp.float32), so_far, back(by_y)[0]), None

    none_yet = {name: jnp.zeros(w.shape, jnp.float32) for name, w in weights.items()}
    by_weights, _ = lax.scan(take, none_yet, (x, dy))
    gradients = [by_weights[name].astype(jnp.bfloat16).astype(jnp.float32) for name in NAMES]
    gradients = clipped(gradients, sum(jnp.sum(g * g) for g in gradients), sum(g.size for g in gradients))
    new = [
        adamw(w.astype(jnp.float32), m, v, g)
        for w, m, v, g in zip((w_gate, w_up, w_down), (m_w_gate, m_w_up, m_w_down), (v_w_gate, v_w_up, v_w_down), gradients, strict=True)
    ]
    return tuple(one[which] for which in range(3) for one in new)
```

```python
import functools

import jax
import jax.numpy as jnp
from jax import lax
from jax.experimental import pallas as pl
from jax.experimental.pallas import tpu as pltpu
from jax.sharding import PartitionSpec as P

BF16, F32 = jnp.bfloat16, jnp.float32
MESH = pl.DeviceIdType.MESH
LANES = 128
TILE = 256
ROWS = 256
SLOTS = 4
LAG2, LAG3 = 2, 3


def dot(a, b):
    return jnp.dot(a, b, preferred_element_type=F32)


def dot_t(a, b):
    return lax.dot_general(a, b, (((1,), (1,)), ((), ())), preferred_element_type=F32)


def sigmoid(x):
    return 0.5 * jnp.tanh(0.5 * x) + 0.5


def step_kernel(
    n, x_hbm, dy_hbm, wg_hbm, wu_hbm, wd_hbm, gg_hbm, gu_hbm, gd_hbm, factor_ref,
    x_v, dy_v, h_v, a_v, at_v, ct_v, ctt_v, acc, wg, wu, wd, gs, us, ds, own, drecv, h1, h2, gg, gu, gd, ss, ss_all,
    in_sem, w_sem, out_sem, d_send, d_recv, h1_send, h1_recv, h2_send, h2_recv, cr_p, cr_n, ss_send, ss_recv,
):
    layers, width, units = wg_hbm.shape
    share = width // n
    per = units // n
    chunks = per // LANES
    chunk = n * LANES
    total = layers * chunks
    block = own.shape[3]
    half = block // 2
    chips = n // 2
    tiles = chunk // TILE

    me = lax.axis_index("dp")
    c, k = lax.div(me, 2), lax.rem(me, 2)
    c_right, c_left, c_far = lax.rem(c + 1, chips), lax.rem(c + chips - 1, chips), lax.rem(c + 2, chips)
    right, left, other = c_right * 2 + k, c_left * 2 + k, c * 2 + (1 - k)

    barrier = pltpu.get_barrier_semaphore()
    for away in range(1, n):
        pl.semaphore_signal(barrier, inc=1, device_id={"dp": lax.rem(me + away, n)}, device_id_type=MESH)

    def fetch(t):
        slot, number, j = lax.rem(t, 2), lax.rem(lax.div(t, chunks), layers), lax.rem(t, chunks)
        for i in range(n):
            at = pl.ds(pl.multiple_of(i * per + j * LANES, LANES), LANES)
            here = pl.ds(i * LANES, LANES)
            pltpu.make_async_copy(wg_hbm.at[number, :, at], wg.at[slot, :, here], w_sem.at[0, slot]).start()
            pltpu.make_async_copy(wu_hbm.at[number, :, at], wu.at[slot, :, here], w_sem.at[1, slot]).start()
            pltpu.make_async_copy(wd_hbm.at[number, at, :], wd.at[slot, here, :], w_sem.at[2, slot]).start()

    def fetched(t):
        slot = lax.rem(t, 2)
        pltpu.make_async_copy(wg.at[slot], wg.at[slot], w_sem.at[0, slot]).wait()
        pltpu.make_async_copy(wu.at[slot], wu.at[slot], w_sem.at[1, slot]).wait()
        pltpu.make_async_copy(wd.at[slot], wd.at[slot], w_sem.at[2, slot]).wait()

    load_x = pltpu.make_async_copy(x_hbm.at[0], x_v, in_sem.at[0])
    load_dy = pltpu.make_async_copy(dy_hbm.at[0], dy_v, in_sem.at[1])
    load_x.start()
    fetch(0)
    load_dy.start()
    load_x.wait()

    tokens = x_v.shape[0]
    blocks = [slice(r, r + ROWS) for r in range(0, tokens, ROWS)]

    def scale_of(wide):
        return lax.rsqrt(jnp.mean(wide * wide, -1, keepdims=True) + 1e-6)

    def normed(src, rows):
        wide = src[rows, :].astype(F32)
        a = (wide * scale_of(wide)).astype(BF16)
        a_v[rows, :] = a
        at_v[:, rows] = a.T

    for rows in blocks:
        normed(x_v, rows)
    acc[...] = jnp.zeros_like(acc)

    def forward(t, _):
        slot = lax.rem(t, 2)
        fetched(t)
        fetch(t + 1)
        for f in range(tiles):
            cols = slice(f * TILE, (f + 1) * TILE)
            gate = dot(a_v[...], wg[slot, :, cols])
            up = dot(a_v[...], wu[slot, :, cols])
            act = (gate * sigmoid(gate) * up).astype(BF16)
            acc[...] += dot(act, wd[slot, cols, :])
        return 0

    lax.fori_loop(0, chunks, forward, 0)
    load_dy.wait()
    for rows in blocks:
        h_v[rows, :] = (x_v[rows, :].astype(F32) + acc[rows, :].astype(BF16).astype(F32)).astype(BF16)
        normed(h_v, rows)
        ct_v[rows, :] = dy_v[rows, :]
        ctt_v[:, rows] = dy_v[rows, :].T
    acc[...] = jnp.zeros_like(acc)
    ss[...] = jnp.zeros_like(ss)
    pl.semaphore_wait(barrier, n - 1)

    def to(src, dst, send, recv, device):
        return pltpu.make_async_remote_copy(src, dst, send, recv, device_id={"dp": device}, device_id_type=MESH)

    def across(s):
        slot = lax.rem(s, SLOTS)
        return to(own.at[slot, 1 - k], drecv.at[slot], d_send.at[slot], d_recv.at[slot], other)

    def hop1(s, way):
        slot = lax.rem(s, SLOTS)
        rows = pl.ds(half, half) if way == 0 else pl.ds(0, half)
        return to(own.at[slot, k, c_far, rows], h1.at[slot, way], h1_send.at[slot, way], h1_recv.at[slot, way], (right, left)[way])

    def hop2(s, way):
        slot = lax.rem(s, SLOTS)
        return to(own.at[slot, k, (c_right, c_left)[way]], h2.at[slot, way], h2_send.at[slot, way], h2_recv.at[slot, way], (right, left)[way])

    def wide(ref):
        return ref[...].astype(F32)

    def t0(s):
        @pl.when(s >= SLOTS)
        def _():
            pl.semaphore_wait(cr_p, 1)

        across(s).start()

    def t1(s):
        slot = lax.rem(s, SLOTS)
        across(s).wait_recv()
        mine = own.at[slot, k, c_far]
        mine[...] = (wide(mine) + wide(drecv.at[slot, c_far])).astype(BF16)

        @pl.when(s >= SLOTS)
        def _():
            for way in range(2):
                pl.semaphore_wait(cr_n.at[way], 1)

        for way in range(2):
            hop1(s, way).start()

    def t2(s):
        slot = lax.rem(s, SLOTS)
        for way in range(2):
            hop1(s, way).wait_recv()
        for way in range(2):
            chip = (c_right, c_left)[way]
            for part in range(2):
                rows = pl.ds(part * half, half)
                mine = own.at[slot, k, chip, rows]
                value = wide(mine) + wide(drecv.at[slot, chip, rows])
                if part == 1 - way:
                    value += wide(h1.at[slot, way])
                mine[...] = value.astype(BF16)
        for way in range(2):
            hop2(s, way).start()

    def t3(s):
        slot = lax.rem(s, SLOTS)
        number, j = layers - 1 - lax.div(s, chunks), lax.rem(s, chunks)
        for way in range(2):
            hop2(s, way).wait_recv()
        lane = pl.ds(pl.multiple_of(j * LANES, LANES), LANES)

        def summed(start, size):
            rows = pl.ds(start, size)
            value = wide(own.at[slot, k, c, rows]) + wide(drecv.at[slot, c, rows])
            value = (value + wide(h2.at[slot, 0, rows]) + wide(h2.at[slot, 1, rows])).astype(BF16)
            return value, jnp.sum((value.astype(F32) ** 2).reshape(size // 8, 8, LANES), 0)

        value, squares = summed(0, width)
        gd[number, lane, :] = value.astype(F32).T.astype(BF16)
        for base, g in ((width, gg), (width + n * share, gu)):
            for i in range(n):
                value, more = summed(base + i * share, share)
                g[number, :, pl.ds(pl.multiple_of(i * per + j * LANES, LANES), LANES)] = value
                squares += more
        ss[...] += squares
        across(s).wait_send()
        for way in range(2):
            hop1(s, way).wait_send()
            hop2(s, way).wait_send()

        @pl.when(s + SLOTS < total)
        def _():
            pl.semaphore_signal(cr_p, inc=1, device_id={"dp": other}, device_id_type=MESH)
            pl.semaphore_signal(cr_n.at[0], inc=1, device_id={"dp": left}, device_id_type=MESH)
            pl.semaphore_signal(cr_n.at[1], inc=1, device_id={"dp": right}, device_id_type=MESH)

        @pl.when(j == chunks - 1)
        def _():
            for i, (src, dst) in enumerate(((gg, gg_hbm), (gu, gu_hbm), (gd, gd_hbm))):
                pltpu.make_async_copy(src.at[number], dst.at[number], out_sem.at[i, number]).start()

    def ticks(s):
        @pl.when(jnp.logical_and(s >= 2, s <= total))
        def _():
            t1(s - 1)

        @pl.when(jnp.logical_and(s >= LAG2, s < total + LAG2))
        def _():
            t2(s - LAG2)

        @pl.when(s >= LAG3)
        def _():
            t3(s - LAG3)

    def store(slot, f, base, value):
        value = value.astype(BF16)
        for i in range(TILE // LANES):
            at = f * (TILE // LANES) + i
            part = value[:, i * LANES : (i + 1) * LANES]
            if base == 0:
                own[slot, at % 2, at // 2, 0:width, :] = part
            else:
                first = base + at * share
                for o in range(n):
                    own[slot, o % 2, o // 2, first : first + share, :] = part[o * share : (o + 1) * share, :]

    def backward(last, first, s, _):
        t = s + chunks
        slot, keep = lax.rem(t, 2), lax.rem(s, SLOTS)
        fetched(t)
        if first:

            @pl.when(s < total - 1)
            def _():
                fetch(t + 1)

        else:
            fetch(t + 1)
        for f in range(tiles):
            cols = slice(f * TILE, (f + 1) * TILE)
            gs[...] = dot(a_v[...], wg[slot, :, cols])
            us[...] = dot(a_v[...], wu[slot, :, cols])
            ds[...] = dot_t(ct_v[...], wd[slot, cols, :]).astype(BF16)
            gate, up, dact = gs[...], us[...], wide(ds)
            sig = sigmoid(gate)
            silu = gate * sig
            act = (silu * up).astype(BF16)
            dup = (dact * silu).astype(BF16)
            dgate = (dact * up * (sig + silu * (1 - sig))).astype(BF16)
            store(keep, f, 0, dot(ctt_v[...], act))
            store(keep, f, width, dot(at_v[...], dgate))
            store(keep, f, width + n * share, dot(at_v[...], dup))
            if not first:
                acc[...] += dot_t(dgate, wg[slot, :, cols]) + dot_t(dup, wu[slot, :, cols])
            if f == 0:
                ticks(s)
        t0(s)
        if last:

            @pl.when(s == 0)
            def _():
                t1(s)

        return 0

    lax.fori_loop(0, chunks, functools.partial(backward, True, False), 0)
    for rows in blocks:
        u = acc[rows, :].astype(BF16).astype(F32)
        h = h_v[rows, :].astype(F32)
        scale = scale_of(h)
        dh = scale * u - h * (scale * scale * scale * jnp.mean(u * h, -1, keepdims=True))
        ct = (dy_v[rows, :].astype(F32) + dh.astype(BF16).astype(F32)).astype(BF16)
        ct_v[rows, :] = ct
        ctt_v[:, rows] = ct.T
        normed(x_v, rows)
    lax.fori_loop(chunks, total, functools.partial(backward, False, True), 0)

    def drain(s, _):
        ticks(s)
        return 0

    lax.fori_loop(total, total + LAG3, drain, 0)

    def squares_to(away):
        peer = lax.rem(me + away, n)
        return to(ss, ss_all.at[me], ss_send.at[away], ss_recv.at[me], peer)

    for away in range(1, n):
        squares_to(away).start()
    ss_all[me] = ss[...]
    for away in range(1, n):
        peer = lax.rem(me + away, n)
        to(ss, ss_all.at[peer], ss_send.at[away], ss_recv.at[peer], peer).wait_recv()
    everyone = ss_all[0]
    for i in range(1, n):
        everyone += ss_all[i]
    mean = jnp.sum(jnp.sum(everyone, 1, keepdims=True), 0, keepdims=True) / (3.0 * layers * width * units)
    factor_ref[...] = jnp.broadcast_to(jnp.minimum(1.0, 0.5 * lax.rsqrt(mean + 1e-30)), factor_ref.shape)
    for away in range(1, n):
        squares_to(away).wait_send()
    for i, (src, dst) in enumerate(((gg, gg_hbm), (gu, gu_hbm), (gd, gd_hbm))):
        for number in range(layers):
            pltpu.make_async_copy(src.at[number], dst.at[number], out_sem.at[i, number]).wait()


def gradients(n, x, dy, w_gate, w_up, w_down):
    layers, width, units = w_gate.shape
    tokens = x.shape[1]
    share, per, chunk = width // n, units // n, n * LANES
    block = width + 2 * n * share
    hbm, vmem = pl.BlockSpec(memory_space=pl.ANY), pl.BlockSpec(memory_space=pltpu.VMEM)
    dma, regular = pltpu.SemaphoreType.DMA, pltpu.SemaphoreType.REGULAR
    return pl.pallas_call(
        functools.partial(step_kernel, n),
        out_shape=[
            jax.ShapeDtypeStruct((layers, share, units), BF16),
            jax.ShapeDtypeStruct((layers, share, units), BF16),
            jax.ShapeDtypeStruct((layers, per, width), BF16),
            jax.ShapeDtypeStruct((8, LANES), F32),
        ],
        in_specs=[hbm] * 5,
        out_specs=[hbm] * 3 + [vmem],
        scratch_shapes=[
            *[pltpu.VMEM((tokens, width), BF16)] * 4,
            pltpu.VMEM((width, tokens), BF16),
            pltpu.VMEM((tokens, width), BF16),
            pltpu.VMEM((width, tokens), BF16),
            pltpu.VMEM((tokens, width), F32),
            pltpu.VMEM((2, width, chunk), BF16),
            pltpu.VMEM((2, width, chunk), BF16),
            pltpu.VMEM((2, chunk, width), BF16),
            pltpu.VMEM((tokens, TILE), F32),
            pltpu.VMEM((tokens, TILE), F32),
            pltpu.VMEM((tokens, TILE), BF16),
            pltpu.VMEM((SLOTS, 2, n // 2, block, LANES), BF16),
            pltpu.VMEM((SLOTS, n // 2, block, LANES), BF16),
            pltpu.VMEM((SLOTS, 2, block // 2, LANES), BF16),
            pltpu.VMEM((SLOTS, 2, block, LANES), BF16),
            pltpu.VMEM((layers, share, units), BF16),
            pltpu.VMEM((layers, share, units), BF16),
            pltpu.VMEM((layers, per, width), BF16),
            pltpu.VMEM((8, LANES), F32),
            pltpu.VMEM((n, 8, LANES), F32),
            dma((2,)),
            dma((3, 2)),
            dma((3, layers)),
            dma((SLOTS,)),
            dma((SLOTS,)),
            dma((SLOTS, 2)),
            dma((SLOTS, 2)),
            dma((SLOTS, 2)),
            dma((SLOTS, 2)),
            regular,
            regular((2,)),
            dma((n,)),
            dma((n,)),
        ],
        compiler_params=pltpu.CompilerParams(collective_id=0, has_side_effects=True, vmem_limit_bytes=63 * 1024 * 1024),
        name="step",
    )(x, dy, w_gate, w_up, w_down)


def adamw(w, m, v, g):
    m = 0.9 * m + 0.1 * g
    v = 0.95 * v + 0.05 * g * g
    step = m * lax.rsqrt(v + 1e-8) + 0.1 * w
    return (w - 0.02 * step).astype(BF16), m, v


def solution(mesh):
    n = mesh.shape["dp"]

    def on_a_device(x, dy, *arrays):
        weights, ms, vs = (arrays[i : i + 3] for i in (0, 3, 6))
        *grads, factor = gradients(n, x, dy, *weights)
        factor = factor[0, 0]
        me = lax.axis_index("dp")
        new = []
        for w, m, v, g in zip(weights, ms, vs, grads, strict=True):
            rows = w.shape[1] // n
            mine = lax.dynamic_slice_in_dim(w, me * rows, rows, 1)
            w, m, v = adamw(mine.astype(F32), m, v, g.astype(F32) * factor)
            new.append((lax.all_gather(w, "dp", axis=1, tiled=True), m, v))
        return tuple(one[which] for which in range(3) for one in new)

    one, every, block = P(("rep", "dp"), None, None), P(None, None, None), P(None, "dp", None)
    return jax.shard_map(
        on_a_device,
        mesh=mesh,
        in_specs=(one, one, *[every] * 3, *[block] * 6),
        out_specs=(*[P("rep", None, None)] * 3, *[P("rep", "dp", None)] * 6),
        check_vma=False,
    )
```
